32 devices in a mesh: blk: 16 (over z, y, x), fsdp: 2 (over core).
Axes of the slice: x: 2, y: 2, z: 4, core: 2. Of those that a mesh axis runs over, the one named last changes fastest.
Arguments:
- hidden_in: bfloat16 [2, 8192, 2048], P('fsdp', 'blk'), may hold values from -6 to 6
- w_query: bfloat16 [2048, 128], P('fsdp'), may hold values from -0.125 to 0.125
- query_gain: float32 [128], replicated, may hold values from 0.1 to 1.9
- key_rows: bfloat16 [2, 8192, 128], P('fsdp', 'blk'), may hold values from -4 to 4
- value_rows: bfloat16 [2, 8192, 128], P('fsdp', 'blk'), may hold values from -6 to 6
- grad_out: bfloat16 [2, 8192, 128], P('fsdp', 'blk'), may hold values from -6 to 6
- logsumexp: float32 [2, 8192], P('fsdp', 'blk'), may hold values from 4 to 8
- row_delta: float32 [2, 8192], P('fsdp', 'blk'), may hold values from -6 to 6
- doc_ids: int32 [2, 8192], P('fsdp', 'blk'), may hold values from 0 to 7, never falling along the last dimension, each value on 1 to 4096 neighbouring positions
Outputs:
- grad_hidden: bfloat16 [2, 8192, 2048], P('fsdp', 'blk')
- grad_keys: bfloat16 [2, 8192, 128], P('fsdp', 'blk')
- grad_values: bfloat16 [2, 8192, 128], P('fsdp', 'blk')
- grad_wquery: float32 [2048, 128], P('fsdp')
The draws below stay inside these ranges and needn't reach their ends.
Inputs may be any that keep to these rules, and one draw needn't show every extreme that they name: `doc_ids`: along each sequence the document numbers never fall; each document has 1 to 4096 tokens.
All inputs are finite; a program needn't handle non-finite values.
Results may differ from the reference program's by a relative error of at most 0.0097.
Values may be sent and summed in bfloat16 or wider, within the bound.
No kernel may reach another device: no remote copies, remote signals or barrier semaphores. Data moves between devices by JAX's collectives and lax.ppermute only.
A program may use at most 64 MiB of HBM per device.

```python
import math
import jax
import jax.numpy as jnp
import numpy as np
from jax import lax

D = 2048
HD = 128
TOK_DEV = 512
ROUNDS = 8
SEQS = 2
LEN = 8192
DOCS = 8
DOC_MOST = 4096
N_BLK = 16


def with_spikes(drawn, own_key, source, target, blocks, factor):
    owner, partner = [(jnp.arange(drawn.shape[axis_at]) // (drawn.shape[axis_at] // blocks)).reshape([-1 if axis == axis_at else 1 for axis in range(drawn.ndim)]) for axis_at in (source, target)]
    chosen = jax.random.permutation(own_key, blocks)[partner]
    strong = (owner == chosen) | (owner == (partner + blocks // 2) % blocks)
    return jnp.where(strong, factor * drawn, drawn)


def steps_of(rng, extent, pieces, least, high):
    def one(dim, shards_of):
        heights = jax.random.uniform(jax.random.fold_in(jax.random.fold_in(rng, 6), dim), (shards_of,), jnp.float32, least / len(pieces), high / len(pieces))
        return jnp.repeat(jnp.exp(heights), extent[dim] // shards_of).reshape((-1,) + (1,) * (len(extent) - dim - 1))

    gain = one(*pieces[0])
    for cut in pieces[1:]:
        gain = gain * one(*cut)
    return gain


def profile(count, total, most, slope):
    weights = [(1 << 20) // math.isqrt(rank ** slope) + 1 for rank in range(2, count + 1)]
    surplus, counts = total - most - (count - 1), [1] * (count - 1)
    while surplus > 0:
        free = [i for i in range(count - 1) if counts[i] < most]
        pool, remaining = sum([weights[i] for i in free]), surplus
        for i in free:
            extra = min(most - counts[i], max(1, remaining * weights[i] // pool), surplus)
            counts[i] = counts[i] + extra
            surplus = surplus - extra
    return np.array([most] + counts)


def uneven(stream_key, amount, total, limit, slope):
    if amount == 2:
        one = jax.random.randint(stream_key, (), max(1, total - limit), min(limit, total - 1) + 1)
        return jnp.stack([one, total - one])
    lengths = jnp.asarray(profile(amount, total, limit, slope), jnp.int32)
    couples = (amount - 1) // 2
    giver, receiver = lengths[1:1 + 2 * couples:2], lengths[2:2 + 2 * couples:2]
    room = jnp.minimum(giver - 1, limit - receiver)
    shifted = jax.random.randint(jax.random.fold_in(stream_key, 1), (couples,), 0, 1 << 20) % (room + 1)
    lengths = lengths.at[1:1 + 2 * couples:2].set(giver - shifted).at[2:2 + 2 * couples:2].set(receiver + shifted)
    return lengths[jax.random.permutation(jax.random.fold_in(stream_key, 2), amount)]


def bell_draw(stream_key, extent, deviation, limit, split=(), held_as=jnp.bfloat16):
    loudness = steps_of(stream_key, extent, split, -0.22, 0.18) if split else 1.0
    entries = jax.random.normal(stream_key, extent, jnp.float32) * deviation * loudness
    return jnp.minimum(jnp.maximum(entries, -limit), limit).astype(held_as)


def noise_with(rng, extent, scale, reach, pieces, heavy, kind=jnp.bfloat16):
    values = scale * jax.random.normal(rng, extent, jnp.float32)
    if pieces:
        values = values * steps_of(rng, extent, pieces, -0.22, 0.18)
    return jnp.clip(with_spikes(values, jax.random.fold_in(rng, 3), *heavy), -reach, reach).astype(kind)


def setup_inputs(seed: int = 0) -> dict:
    splits = jax.random.split(jax.random.key(seed), 10)
    hidden_in = noise_with(splits[0], (SEQS, LEN, D), 1.0, 6.0, ((0, 2), (1, 16)), (1, 2, 16, 2.0))
    w_query = bell_draw(splits[1], (D, HD), D ** -0.5, 0.125, ((0, 2),))
    query_gain = jnp.clip(1.0 + 0.18 * jax.random.normal(splits[2], (HD,), jnp.float32), 0.1, 1.9)
    key_rows = bell_draw(splits[3], (SEQS, LEN, HD), 1.0, 4.0, ((0, 2), (1, 16)))
    value_rows = bell_draw(splits[4], (SEQS, LEN, HD), 1.0, 6.0, ((0, 2), (1, 16)))
    grad_out = bell_draw(splits[5], (SEQS, LEN, HD), 1.0, 6.0, ((0, 2), (1, 16)))
    logsumexp = jnp.clip(4.0 + 4.0 * jax.random.uniform(splits[6], (SEQS, LEN), jnp.float32) ** steps_of(splits[6], (SEQS, LEN), ((0, 2), (1, 16)), -0.2, 0.2), 4.0, 8.0)
    row_delta = bell_draw(splits[7], (SEQS, LEN), 1.0, 6.0, ((0, 2), (1, 16)), jnp.float32)
    doc_ids = jax.vmap(lambda own: jnp.searchsorted(jnp.cumsum(uneven(own, DOCS, LEN, DOC_MOST, 2)), jnp.arange(LEN), side="right"))(jax.random.split(splits[8], SEQS)).reshape((SEQS, LEN)).astype(jnp.int32)
    return dict(hidden_in=hidden_in, w_query=w_query, query_gain=query_gain, key_rows=key_rows, value_rows=value_rows, grad_out=grad_out, logsumexp=logsumexp, row_delta=row_delta, doc_ids=doc_ids)


def reference(hidden_in, w_query, query_gain, key_rows, value_rows, grad_out, logsumexp, row_delta, doc_ids):
    score_scale = HD ** (-0.5)
    span = ROUNDS * TOK_DEV
    margin = (ROUNDS - 1) * TOK_DEV
    lower_tri = jnp.arange(TOK_DEV, dtype=jnp.int32)[:, None] + margin >= jnp.arange(span, dtype=jnp.int32)[None, :]
    hidden_list = []
    keys_list = []
    values_list = []
    weight_total = jnp.zeros((D, HD), jnp.float32)
    for seq_index in range(SEQS):
        inputs = hidden_in[seq_index]
        q_pre = jnp.dot(inputs, w_query, preferred_element_type=jnp.float32)
        inverse = lax.rsqrt(lax.optimization_barrier(jnp.mean(q_pre * q_pre, axis=-1, keepdims=True)) + 1e-06)
        normed = q_pre * inverse
        query = (normed * query_gain).astype(jnp.bfloat16)
        key_pad = jnp.concatenate([jnp.zeros((margin, HD), key_rows.dtype), key_rows[seq_index]], 0)
        value_pad = jnp.concatenate([jnp.zeros((margin, HD), value_rows.dtype), value_rows[seq_index]], 0)
        doc_pad = jnp.concatenate([-jnp.ones((margin,), jnp.int32), doc_ids[seq_index].astype(jnp.int32)], 0)
        outgrad = grad_out[seq_index]
        lse_row = logsumexp[seq_index]
        delta_row = row_delta[seq_index]
        doc_row = doc_ids[seq_index].astype(jnp.int32)

        def block_step(carry, block):
            keys_acc, values_acc = carry
            start = (block * TOK_DEV).astype(jnp.int32)
            q_block = lax.dynamic_slice_in_dim(query, start, TOK_DEV, 0)
            o_block = lax.dynamic_slice_in_dim(outgrad, start, TOK_DEV, 0)
            l_block = lax.dynamic_slice_in_dim(lse_row, start, TOK_DEV, 0)
            d_block = lax.dynamic_slice_in_dim(delta_row, start, TOK_DEV, 0)
            s_block = lax.dynamic_slice_in_dim(doc_row, start, TOK_DEV, 0)
            k_window = lax.dynamic_slice_in_dim(key_pad, start, span, 0)
            v_window = lax.dynamic_slice_in_dim(value_pad, start, span, 0)
            s_window = lax.dynamic_slice_in_dim(doc_pad, start, span, 0)
            allowed = (s_block[:, None] == s_window[None, :]) & lower_tri
            scores = lax.dot_general(q_block, k_window, (((1,), (1,)), ((), ())), preferred_element_type=jnp.float32) * score_scale
            attn_prob = jnp.exp(jnp.where(allowed, scores - l_block[:, None], -1e+30))
            grad_prob = lax.dot_general(o_block, v_window, (((1,), (1,)), ((), ())), preferred_element_type=jnp.float32)
            grad_score = attn_prob * (grad_prob - d_block[:, None])
            prob_half = attn_prob.astype(jnp.bfloat16)
            score_half = grad_score.astype(jnp.bfloat16)
            query_term = jnp.dot(score_half, k_window, preferred_element_type=jnp.float32)
            key_term = lax.dot_general(score_half, q_block, (((0,), (0,)), ((), ())), preferred_element_type=jnp.float32)
            value_term = lax.dot_general(prob_half, o_block, (((0,), (0,)), ((), ())), preferred_element_type=jnp.float32)
            keys_acc = lax.dynamic_update_slice_in_dim(keys_acc, lax.dynamic_slice_in_dim(keys_acc, start, span, 0) + key_term, start, 0)
            values_acc = lax.dynamic_update_slice_in_dim(values_acc, lax.dynamic_slice_in_dim(values_acc, start, span, 0) + value_term, start, 0)
            return ((keys_acc, values_acc), query_term)
        zeros_pad = jnp.zeros((margin + LEN, HD), jnp.float32)
        (keys_acc, values_acc), query_blocks = lax.scan(block_step, (zeros_pad, zeros_pad), jnp.arange(N_BLK, dtype=jnp.int32))
        grad_query = query_blocks.reshape(LEN, HD) * score_scale
        keys_list.append((keys_acc[margin:] * score_scale).astype(jnp.bfloat16))
        values_list.append(values_acc[margin:].astype(jnp.bfloat16))
        scaled = grad_query * query_gain
        grad_pre = (inverse * (scaled - normed * lax.optimization_barrier(jnp.mean(scaled * normed, axis=-1, keepdims=True)))).astype(jnp.bfloat16)
        hidden_list.append(lax.dot_general(grad_pre, w_query, (((1,), (1,)), ((), ())), preferred_element_type=jnp.float32).astype(jnp.bfloat16))
        weight_total = weight_total + lax.dot_general(inputs, grad_pre, (((0,), (0,)), ((), ())), preferred_element_type=jnp.float32)
    return (jnp.stack(hidden_list), jnp.stack(keys_list), jnp.stack(values_list), weight_total)
```

```python
import functools
import math

import jax
import jax.numpy as jnp
from jax import lax
from jax.experimental import pallas as pl
from jax.experimental.pallas import tpu as pltpu
from jax.sharding import PartitionSpec as P

ROUNDS = 8
LOG2E = 1.4426950408889634
BF = jnp.bfloat16
F32 = jnp.float32
T_CHUNK = 256


def shifted(value, by):
    size = lax.axis_size("blk")
    pairs = [(i, i + by) for i in range(size) if 0 <= i + by < size]
    return lax.ppermute(value, "blk", pairs)


def turned(value, by, group):
    size = lax.axis_size("blk")
    pairs = [(i, i - i % group + (i + by) % group) for i in range(size)]
    return lax.ppermute(value, "blk", pairs)


def pieces(x):
    hi = lax.reduce_precision(x, 8, 7)
    rest = x - hi
    mid = lax.reduce_precision(rest, 8, 7)
    return [hi.astype(BF), mid.astype(BF), (rest - mid).astype(BF)]


def rows_of(vectors, width, total):
    flat = jnp.concatenate(vectors).reshape(-1, width)
    return jnp.pad(flat, ((0, total - flat.shape[0]), (0, 0)))


def dot_nt(a, b):
    return lax.dot_general(a, b, (((1,), (1,)), ((), ())), preferred_element_type=F32)


def dot_nn(a, b):
    return lax.dot_general(a, b, (((1,), (0,)), ((), ())), preferred_element_type=F32)


def attention_kernel(group, far, tokens, width, r_ref, *refs):
    sizes = [group, group, far + 1]
    q_refs, o_refs, kv_refs = (
        refs[: group],
        refs[group : 2 * group],
        refs[2 * group : sum(sizes)],
    )
    rest = refs[sum(sizes) :]
    dq_refs, dkv_refs = rest[:group], rest[group : group + far + 1]
    kt_sc, docs_sc, dk_acc, dv_acc, k_sc, v_sc = rest[group + far + 1 :]
    r = r_ref[0]
    per = tokens // width
    scale = width ** (-0.5)

    for s in range(far + 1):
        k_sc[s] = kv_refs[s][:tokens]
        v_sc[s] = kv_refs[s][tokens : 2 * tokens]
        kt_sc[s] = kv_refs[s][:tokens].astype(F32).T.astype(BF)
        docs = kv_refs[s][2 * tokens :].astype(F32)
        for j in range(per):
            row = jnp.broadcast_to(docs[j : j + 1, :], (width, width))
            docs_sc[s, j * width : (j + 1) * width, :] = row.T
        dk_acc[s] = jnp.zeros((tokens, width), F32)
        dv_acc[s] = jnp.zeros((tokens, width), F32)

    def row_of(aux, at):
        return jnp.concatenate([aux[at + j : at + j + 1, :] for j in range(per)], axis=1)

    for k in range(group):
        q = q_refs[k][...]
        o = o_refs[k][:tokens]
        aux = o_refs[k][tokens:].astype(F32)
        part = [row_of(aux, i * per) for i in range(7)]
        lse = (part[0] + part[1] + part[2]) * LOG2E
        delta = part[3] + part[4] + part[5]
        docs_q = part[6]
        dqt = jnp.zeros((width, tokens), F32)
        for j in range(far):
            if j > 0:
                s = j
            elif k == 0:
                s = 0
            else:
                s = jnp.where(r >= k, far, 0)
            for c in range(0, tokens, T_CHUNK):
                rows = slice(c, c + T_CHUNK)
                scores = dot_nt(k_sc[s, rows, :], q)
                grad_prob = dot_nt(v_sc[s, rows, :], o)
                allowed = docs_sc[s, rows, :1] == docs_q
                if j == 0 and k == 0:
                    t_at = c + lax.broadcasted_iota(jnp.int32, (T_CHUNK, tokens), 0)
                    i_at = lax.broadcasted_iota(jnp.int32, (T_CHUNK, tokens), 1)
                    allowed = allowed & (t_at <= i_at)
                prob = jnp.where(allowed, jnp.exp2(scores * (scale * LOG2E) - lse), 0.0)
                dscore = (prob * (grad_prob - delta)).astype(BF)
                dv_acc[s, rows, :] += dot_nn(prob.astype(BF), o)
                dk_acc[s, rows, :] += dot_nn(dscore, q)
                dqt += dot_nn(kt_sc[s, :, rows], dscore)
        dq_refs[k][...] = (dqt.T * scale).astype(dq_refs[k].dtype)

    for s in range(far + 1):
        dkv_refs[s][:tokens] = (dk_acc[s] * scale).astype(dkv_refs[s].dtype)
        dkv_refs[s][tokens:] = dv_acc[s].astype(dkv_refs[s].dtype)


def attention(group, far, tokens, width, r, q_list, o_list, kv_list):
    vmem = pl.BlockSpec(memory_space=pltpu.VMEM)
    pairs = group * far
    dq_shapes = [
        jax.ShapeDtypeStruct((tokens, width), F32 if k == 0 else BF) for k in range(group)
    ]
    dkv_shapes = [
        jax.ShapeDtypeStruct((2 * tokens, width), F32 if s == 0 else BF) for s in range(far + 1)
    ]
    out = pl.pallas_call(
        functools.partial(attention_kernel, group, far, tokens, width),
        out_shape=dq_shapes + dkv_shapes,
        in_specs=[pl.BlockSpec(memory_space=pltpu.SMEM)] + [vmem] * (2 * group + far + 1),
        out_specs=[vmem] * (group + far + 1),
        scratch_shapes=[
            pltpu.VMEM((far + 1, width, tokens), BF),
            pltpu.VMEM((far + 1, tokens, width), F32),
            pltpu.VMEM((far + 1, tokens, width), F32),
            pltpu.VMEM((far + 1, tokens, width), F32),
            pltpu.VMEM((far + 1, tokens, width), BF),
            pltpu.VMEM((far + 1, tokens, width), BF),
        ],
        compiler_params=pltpu.CompilerParams(vmem_limit_bytes=48 * 1024 * 1024),
        cost_estimate=pl.CostEstimate(
            flops=pairs * 10 * tokens * tokens * width,
            bytes_accessed=8 * 1024 * 1024,
            transcendentals=pairs * tokens * tokens,
        ),
        name="attention",
    )(r, *q_list, *o_list, *kv_list)
    return out[:group], out[group:]


def local(
    hidden_in, w_query, query_gain, key_rows, value_rows, grad_out, logsumexp, row_delta, doc_ids
):
    inputs = hidden_in[0]
    tokens, width = key_rows.shape[1:]
    blocks = lax.axis_size("blk")
    halves = lax.axis_size("fsdp")
    group = math.gcd(blocks, max(1, ROUNDS // 2))
    far = ROUNDS // group
    r = (lax.axis_index("blk") % group).astype(jnp.int32)[None]

    per = tokens // width
    docs = (doc_ids[0] + 1).astype(BF)
    kv_own = jnp.concatenate(
        [key_rows[0], value_rows[0], rows_of([docs], width, -(-per // 16) * 16)]
    )
    kv_list = [kv_own] + [shifted(kv_own, group * s) for s in range(1, far + 1)]
    aux = rows_of(
        pieces(logsumexp[0]) + pieces(row_delta[0]) + [docs], width, -(-7 * per // 16) * 16
    )
    o_own = jnp.concatenate([grad_out[0], aux])
    o_list = [o_own] + [turned(o_own, k, group) for k in range(1, group)]

    projection = lax.all_gather(w_query, "fsdp", axis=0, tiled=True)
    q_pre = jnp.dot(inputs, projection, preferred_element_type=F32)
    inverse = lax.rsqrt(jnp.mean(q_pre * q_pre, axis=-1, keepdims=True) + 1e-06)
    normed = q_pre * inverse
    query = (normed * query_gain).astype(BF)
    q_list = [query] + [turned(query, k, group) for k in range(1, group)]

    dq_list, dkv_list = attention(group, far, tokens, width, r, q_list, o_list, kv_list)

    grad_query = dq_list[0]
    for k in range(1, group):
        grad_query = grad_query + turned(dq_list[k], -k, group).astype(F32)
    scaled = grad_query * query_gain
    grad_pre = (
        inverse * (scaled - normed * jnp.mean(scaled * normed, axis=-1, keepdims=True))
    ).astype(BF)
    weight_term = lax.dot_general(
        inputs, grad_pre, (((0,), (0,)), ((), ())), preferred_element_type=F32
    ).astype(BF)
    grad_hidden = dot_nt(grad_pre, projection).astype(BF)

    grad_kv = dkv_list[0]
    for s in range(1, far + 1):
        grad_kv = grad_kv + shifted(dkv_list[s], -group * s).astype(F32)
    grad_kv = grad_kv.astype(BF)

    owned = weight_term.shape[0] // halves
    share = -(-owned // blocks)
    terms = weight_term.reshape(halves, owned, width)
    if share * blocks != owned:
        terms = jnp.pad(terms, ((0, 0), (0, share * blocks - owned), (0, 0)))
    terms = terms.reshape(halves * blocks * share, width)
    got = lax.all_to_all(terms, ("fsdp", "blk"), 0, 0, tiled=True)
    mine = jnp.sum(got.reshape(halves * blocks, share, width).astype(F32), axis=0)
    mine = mine.astype(BF)
    everywhere = jnp.broadcast_to(mine[None], (blocks, share, width)).reshape(-1, width)
    total = lax.all_to_all(everywhere, "blk", 0, 0, tiled=True)
    grad_wquery = total[:owned].astype(F32)
    return (grad_hidden[None], grad_kv[None, :tokens], grad_kv[None, tokens:], grad_wquery)


def solution(mesh):
    return jax.shard_map(
        local,
        mesh=mesh,
        in_specs=(
            P("fsdp", "blk", None),
            P("fsdp", None),
            P(),
            P("fsdp", "blk", None),
            P("fsdp", "blk", None),
            P("fsdp", "blk", None),
            P("fsdp", "blk"),
            P("fsdp", "blk"),
            P("fsdp", "blk"),
        ),
        out_specs=(
            P("fsdp", "blk", None),
            P("fsdp", "blk", None),
            P("fsdp", "blk", None),
            P("fsdp", None),
        ),
        check_vma=False,
    )
```

```python
import functools
import math

import jax
import jax.numpy as jnp
from jax import lax
from jax.experimental import pallas as pl
from jax.experimental.pallas import tpu as pltpu
from jax.sharding import PartitionSpec as P


ROUNDS = 8
LOG2E = 1.4426950408889634
BF = jnp.bfloat16
F32 = jnp.float32
T_CHUNK = 256
PACK_MIB = 63.4
ATTENTION_MIB = 16


def shifted(value, by):
    size = lax.axis_size("blk")
    pairs = [(i, i + by) for i in range(size) if 0 <= i + by < size]
    return lax.ppermute(value, "blk", pairs)


def turned(value, by, group):
    size = lax.axis_size("blk")
    pairs = [(i, i - i % group + (i + by) % group) for i in range(size)]
    return lax.ppermute(value, "blk", pairs)


def vmem_specs(count):
    return [pl.BlockSpec(memory_space=pltpu.VMEM)] * count


def params(mib):
    return pltpu.CompilerParams(vmem_limit_bytes=int(mib * 1024 * 1024))


def dot_nt(a, b):
    return lax.dot_general(a, b, (((1,), (1,)), ((), ())), preferred_element_type=F32)


def dot_nn(a, b):
    return lax.dot_general(a, b, (((1,), (0,)), ((), ())), preferred_element_type=F32)


def hbm_specs(count):
    return [pl.BlockSpec(memory_space=pltpu.HBM)] * count


def whole_specs(arrays):
    return [pl.BlockSpec(x.shape, lambda n=len(x.shape): (0,) * n) for x in arrays]


def fetched(pairs, sems):
    copies = [pltpu.make_async_copy(a, b, sems.at[i]) for i, (a, b) in enumerate(pairs)]
    for copy in copies:
        copy.start()
    return copies


def pack_kernel(
    k_ref, v_ref, o_ref, lse_ref, delta_ref, docs_ref, kv_out, o_out,
    lse_sc, delta_sc, docs_sc, sems,
):
    tokens, width = k_ref.shape
    copies = fetched(
        [
            (docs_ref, docs_sc),
            (lse_ref, lse_sc),
            (delta_ref, delta_sc),
            (k_ref, kv_out.at[:tokens]),
            (v_ref, kv_out.at[tokens : 2 * tokens]),
            (o_ref, o_out.at[:tokens]),
        ],
        sems,
    )
    for copy in copies[:3]:
        copy.wait()
    docs = (docs_sc[...] + 1).astype(F32)
    spare = kv_out.shape[0] - 2 * tokens - docs.shape[0]
    kv_out[2 * tokens :] = jnp.concatenate(
        [docs] + [jnp.zeros((spare, width), F32)] * (spare > 0)
    ).astype(BF)
    rows = []
    for ref in (lse_sc, delta_sc):
        rest = ref[...]
        for _ in range(3):
            piece = rest.astype(BF).astype(F32)
            rows.append(piece)
            rest = rest - piece
    rows.append(docs)
    spare = o_out.shape[0] - tokens - 7 * docs.shape[0]
    o_out[tokens:] = jnp.concatenate(
        rows + [jnp.zeros((spare, width), F32)] * (spare > 0)
    ).astype(BF)
    for copy in copies[3:]:
        copy.wait()


def query_kernel(h_ref, w_ref, gain_ref, query_out, q_pre_out):
    q_pre = dot_nn(h_ref[...], w_ref[...])
    inverse = lax.rsqrt(jnp.mean(q_pre * q_pre, axis=-1, keepdims=True) + 1e-06)
    q_pre_out[...] = q_pre
    query_out[...] = (q_pre * inverse * gain_ref[...]).astype(BF)


def row_data(o_ref, tokens, per):
    aux = o_ref[tokens:].astype(F32)
    part = []
    for at in range(0, 7 * per, per):
        part.append(
            jnp.concatenate([aux[at + j : at + j + 1, :] for j in range(per)], axis=1)
        )
    lse = (part[0] + part[1] + part[2]) * LOG2E
    return lse, part[3] + part[4] + part[5], part[6]


def stage_keys(kv_ref, s, tokens, width, k_sc, v_sc, kt_sc, docs_sc, with_kt):
    k_sc[s] = kv_ref[:tokens]
    v_sc[s] = kv_ref[tokens : 2 * tokens]
    if with_kt:
        kt_sc[s] = kv_ref[:tokens].astype(F32).T.astype(BF)
    docs = kv_ref[2 * tokens :].astype(F32)
    for j in range(tokens // width):
        row = jnp.broadcast_to(docs[j : j + 1, :], (width, width))
        docs_sc[s, j * width : (j + 1) * width, :] = row.T


def probabilities(s, rows, c, q, o, lse, delta, docs_q, diagonal, scale, k_sc, v_sc, docs_sc):
    scores = dot_nt(k_sc[s, rows, :], q)
    grad_prob = dot_nt(v_sc[s, rows, :], o)
    allowed = docs_sc[s, rows, :1] == docs_q
    if diagonal:
        t_at = c + lax.broadcasted_iota(jnp.int32, scores.shape, 0)
        i_at = lax.broadcasted_iota(jnp.int32, scores.shape, 1)
        allowed = allowed & (t_at <= i_at)
    prob = jnp.where(allowed, jnp.exp2(scores * (scale * LOG2E) - lse), 0.0)
    return prob, (prob * (grad_prob - delta)).astype(BF)


def slot(r, k, j, far):
    if j > 0:
        return j
    return 0 if k == 0 else jnp.where(r >= k, far, 0)


def others_kernel(group, far, tokens, width, r_ref, q_ref, *refs):
    o_refs, kv_refs = refs[: group - 1], refs[group - 1 : group + far]
    outs = refs[group + far :]
    dq_refs, dkv_ref, acc = outs[: group - 1], outs[group - 1], outs[group]
    kt_sc, docs_sc, k_sc, v_sc = outs[group + 1 :]
    r = r_ref[0]
    scale = width ** (-0.5)
    for s in range(far + 1):
        stage_keys(kv_refs[s], s, tokens, width, k_sc, v_sc, kt_sc, docs_sc, True)
        acc[s] = jnp.zeros((2 * tokens, width), F32)
    for k in range(1, group):
        q = q_ref[(r - k + group) % group]
        o = o_refs[k - 1][:tokens]
        lse, delta, docs_q = row_data(o_refs[k - 1], tokens, tokens // width)
        dqt = jnp.zeros((width, tokens), F32)
        for j in range(far):
            s = slot(r, k, j, far)
            for c in range(0, tokens, T_CHUNK):
                rows = slice(c, c + T_CHUNK)
                below = slice(tokens + c, tokens + c + T_CHUNK)
                prob, dscore = probabilities(
                    s, rows, c, q, o, lse, delta, docs_q, False, scale, k_sc, v_sc, docs_sc
                )
                acc[s, below, :] += dot_nn(prob.astype(BF), o)
                acc[s, rows, :] += dot_nn(dscore, q)
                dqt += dot_nn(kt_sc[s, :, rows], dscore)
        dq_refs[k - 1][...] = (dqt.T * scale).astype(BF)
    dkv_ref[:tokens] = (acc[far, :tokens] * scale).astype(BF)
    dkv_ref[tokens:] = acc[far, tokens:].astype(BF)


def own_kernel(far, tokens, width, q_ref, o_ref, acc, *refs):
    kv_refs, dq_ref, dkv_refs = refs[:far], refs[far], refs[far + 1 : 2 * far + 1]
    kt_sc, docs_sc, k_sc, v_sc = refs[2 * far + 1 :]
    scale = width ** (-0.5)
    q = q_ref[...]
    o = o_ref[:tokens]
    lse, delta, docs_q = row_data(o_ref, tokens, tokens // width)
    dqt = jnp.zeros((width, tokens), F32)
    for s in range(far):
        stage_keys(kv_refs[s], s, tokens, width, k_sc, v_sc, kt_sc, docs_sc, True)
        for c in range(0, tokens, T_CHUNK):
            rows = slice(c, c + T_CHUNK)
            below = slice(tokens + c, tokens + c + T_CHUNK)
            prob, dscore = probabilities(
                s, rows, c, q, o, lse, delta, docs_q, s == 0, scale, k_sc, v_sc, docs_sc
            )
            dkv_refs[s][below, :] = (acc[s, below, :] + dot_nn(prob.astype(BF), o)).astype(BF)
            dkv_refs[s][rows, :] = ((acc[s, rows, :] + dot_nn(dscore, q)) * scale).astype(BF)
            dqt += dot_nn(kt_sc[s, :, rows], dscore)
    dq_ref[...] = dqt.T * scale


def key_scratch(slots, tokens, width):
    return [
        pltpu.VMEM((slots, width, tokens), BF),
        pltpu.VMEM((slots, tokens, width), F32),
        pltpu.VMEM((slots, tokens, width), BF),
        pltpu.VMEM((slots, tokens, width), BF),
    ]


def cost(pairs, tokens, width):
    return pl.CostEstimate(
        flops=pairs * 10 * tokens * tokens * width,
        bytes_accessed=pairs * 8 * tokens * width,
        transcendentals=pairs * tokens * tokens,
    )


def others(group, far, tokens, width, r, q_all, o_list, kv_list):
    block = jax.ShapeDtypeStruct((tokens, width), BF)
    double = jax.ShapeDtypeStruct((2 * tokens, width), BF)
    sums = jax.ShapeDtypeStruct((far + 1, 2 * tokens, width), F32)
    if group == 1:
        return [], jnp.zeros(double.shape, BF), jnp.zeros(sums.shape, F32)
    out = pl.pallas_call(
        functools.partial(others_kernel, group, far, tokens, width),
        out_shape=[block] * (group - 1) + [double, sums],
        in_specs=[pl.BlockSpec(memory_space=pltpu.SMEM)] + vmem_specs(group + far + 1),
        out_specs=vmem_specs(group + 1),
        scratch_shapes=key_scratch(far + 1, tokens, width),
        compiler_params=params(ATTENTION_MIB),
        cost_estimate=cost((group - 1) * far, tokens, width),
        name="others",
    )(r, q_all, *o_list[1:], *kv_list)
    return out[: group - 1], out[group - 1], out[group]


def own(far, tokens, width, query, o_own, acc, kv_list):
    out = pl.pallas_call(
        functools.partial(own_kernel, far, tokens, width),
        out_shape=[jax.ShapeDtypeStruct((tokens, width), F32)]
        + [jax.ShapeDtypeStruct((2 * tokens, width), BF)] * far,
        in_specs=vmem_specs(far + 3),
        out_specs=vmem_specs(far + 1),
        scratch_shapes=key_scratch(far, tokens, width),
        compiler_params=params(ATTENTION_MIB),
        cost_estimate=cost(far, tokens, width),
        name="own",
    )(query, o_own, acc, *kv_list[:far])
    return out[0], out[1:]


def weight_kernel(parts, h_ref, q_pre_ref, gain_ref, own_ref, *refs):
    grad_query = own_ref[...]
    for ref in refs[:parts]:
        grad_query = grad_query + ref[...].astype(F32)
    pre_out, term_out = refs[parts:]
    q_pre = q_pre_ref[...]
    inverse = lax.rsqrt(jnp.mean(q_pre * q_pre, axis=-1, keepdims=True) + 1e-06)
    normed = q_pre * inverse
    scaled = grad_query * gain_ref[...]
    grad_pre = inverse * (scaled - normed * jnp.mean(scaled * normed, axis=-1, keepdims=True))
    pre_out[...] = grad_pre.astype(BF)
    turned_pre = grad_pre.astype(BF).astype(F32).T.astype(BF)
    columns = h_ref.shape[1]
    step = math.gcd(columns, 512)
    for c in range(0, columns, step):
        term = dot_nn(turned_pre, h_ref[:, c : c + step])
        term_out[c : c + step, :] = term.T.astype(BF)


def sum_kernel(got_ref, out_ref):
    total = got_ref[0].astype(F32)
    for i in range(1, got_ref.shape[0]):
        total = total + got_ref[i].astype(F32)
    total = total.astype(BF)
    for i in range(out_ref.shape[0]):
        out_ref[i] = total


def sum_and_repeat(got, copies):
    share, width = got.shape[1:]
    if share % 16:
        total = jnp.sum(got.astype(F32), axis=0).astype(BF)
        return jnp.broadcast_to(total[None], (copies, share, width))
    return pl.pallas_call(
        sum_kernel,
        out_shape=jax.ShapeDtypeStruct((copies, share, width), BF),
        in_specs=vmem_specs(1),
        out_specs=vmem_specs(1)[0],
        compiler_params=params(8),
        name="sum_and_repeat",
    )(got)


def local(
    hidden_in, w_query, query_gain, key_rows, value_rows, grad_out, logsumexp, row_delta, doc_ids
):
    return step(
        hidden_in[0],
        w_query,
        query_gain[None],
        key_rows[0],
        value_rows[0],
        grad_out[0],
        logsumexp,
        row_delta,
        doc_ids,
    )


def step(inputs, w_query, gain, keys, values, outgrad, logsumexp, row_delta, doc_ids):
    tokens, width = keys.shape
    blocks = lax.axis_size("blk")
    halves = lax.axis_size("fsdp")
    group = math.gcd(blocks, max(1, ROUNDS // 2))
    far = ROUNDS // group
    r = (lax.axis_index("blk") % group).astype(jnp.int32)[None]
    per = tokens // width

    kv_own, o_own = pl.pallas_call(
        pack_kernel,
        out_shape=[
            jax.ShapeDtypeStruct((2 * tokens + -(-per // 16) * 16, width), BF),
            jax.ShapeDtypeStruct((tokens + -(-7 * per // 16) * 16, width), BF),
        ],
        in_specs=hbm_specs(6),
        out_specs=vmem_specs(2),
        scratch_shapes=[
            pltpu.VMEM((per, width), F32),
            pltpu.VMEM((per, width), F32),
            pltpu.VMEM((per, width), jnp.int32),
            pltpu.SemaphoreType.DMA((6,)),
        ],
        compiler_params=params(PACK_MIB),
        name="pack",
    )(
        keys,
        values,
        outgrad,
        logsumexp.reshape(per, width),
        row_delta.reshape(per, width),
        doc_ids.reshape(per, width),
    )
    kv_list = [kv_own] + [shifted(kv_own, group * s) for s in range(far, 0, -1)][::-1]
    o_list = [o_own] + [turned(o_own, k, group) for k in range(1, group)]

    projection = lax.all_gather(w_query, "fsdp", axis=0, tiled=True)
    q_like = jax.ShapeDtypeStruct((tokens, width), F32)
    query, q_pre = pl.pallas_call(
        query_kernel,
        out_shape=[
            jax.ShapeDtypeStruct((tokens, width), BF),
            q_like,
        ],
        in_specs=vmem_specs(1) + whole_specs([projection, gain]),
        out_specs=vmem_specs(1) + whole_specs([q_like]),
        compiler_params=params(8),
        name="query",
    )(inputs, projection, gain)
    groups = [list(range(i, i + group)) for i in range(0, blocks, group)]
    q_all = lax.all_gather(query, "blk", axis_index_groups=groups)

    dq_list, grad_kv, acc = others(group, far, tokens, width, r, q_all, o_list, kv_list)

    dq_back = [turned(dq_list[k - 1], -k, group) for k in range(1, group)]
    back = shifted(grad_kv, -group)
    dq_own, dkv_list = own(far, tokens, width, query, o_own, acc, kv_list)
    grad_pre, weight_term = pl.pallas_call(
        functools.partial(weight_kernel, len(dq_back)),
        out_shape=[
            jax.ShapeDtypeStruct((tokens, width), BF),
            jax.ShapeDtypeStruct((inputs.shape[1], width), BF),
        ],
        in_specs=vmem_specs(1) + whole_specs([q_pre, gain]) + vmem_specs(1 + len(dq_back)),
        out_specs=vmem_specs(2),
        compiler_params=params(16),
        name="weight_term",
    )(inputs, q_pre, gain, dq_own, *dq_back)
    grad_hidden = dot_nt(grad_pre, projection).astype(BF)

    for s in range(far - 1, -1, -1):
        grad_kv = (dkv_list[s].astype(F32) + back.astype(F32)).astype(BF)
        if s > 0:
            back = shifted(grad_kv, -group)

    owned = weight_term.shape[0] // halves
    share = -(-owned // blocks)
    got = lax.all_to_all(weight_term, "fsdp", 0, 0, tiled=True)
    terms = sum_and_repeat(got.reshape(halves, owned, width), 1)[0]
    if share * blocks != owned:
        terms = jnp.pad(terms, ((0, share * blocks - owned), (0, 0)))
    got = lax.all_to_all(terms, "blk", 0, 0, tiled=True)
    everywhere = sum_and_repeat(got.reshape(blocks, share, width), blocks)
    total = lax.all_to_all(everywhere.reshape(-1, width), "blk", 0, 0, tiled=True)
    grad_wquery = total[:owned].astype(F32)
    return (grad_hidden[None], grad_kv[None, :tokens], grad_kv[None, tokens:], grad_wquery)


def solution(mesh):
    return jax.shard_map(
        local,
        mesh=mesh,
        in_specs=(
            P("fsdp", "blk", None),
            P("fsdp", None),
            P(),
            P("fsdp", "blk", None),
            P("fsdp", "blk", None),
            P("fsdp", "blk", None),
            P("fsdp", "blk"),
            P("fsdp", "blk"),
            P("fsdp", "blk"),
        ),
        out_specs=(
            P("fsdp", "blk", None),
            P("fsdp", "blk", None),
            P("fsdp", "blk", None),
            P("fsdp", None),
        ),
        check_vma=False,
    )
```

```python
import functools
import math

import jax
import jax.numpy as jnp
from jax import lax
from jax.experimental import pallas as pl
from jax.experimental.pallas import tpu as pltpu
from jax.sharding import PartitionSpec as P


ROUNDS = 8
LOG2E = 1.4426950408889634
BF = jnp.bfloat16
F32 = jnp.float32
T_CHUNK = 256
PACK_MIB = 63.4
ATTENTION_MIB = 16


def shifted(value, by):
    size = lax.axis_size("blk")
    pairs = [(i, i + by) for i in range(size) if 0 <= i + by < size]
    return lax.ppermute(value, "blk", pairs)


def turned(value, by, group):
    size = lax.axis_size("blk")
    pairs = [(i, i - i % group + (i + by) % group) for i in range(size)]
    return lax.ppermute(value, "blk", pairs)


def vmem_specs(count):
    return [pl.BlockSpec(memory_space=pltpu.VMEM)] * count


def params(mib):
    return pltpu.CompilerParams(vmem_limit_bytes=int(mib * 1024 * 1024))


def dot_nt(a, b):
    return lax.dot_general(a, b, (((1,), (1,)), ((), ())), preferred_element_type=F32)


def dot_nn(a, b):
    return lax.dot_general(a, b, (((1,), (0,)), ((), ())), preferred_element_type=F32)


def hbm_specs(count):
    return [pl.BlockSpec(memory_space=pltpu.HBM)] * count


def whole_specs(arrays):
    return [pl.BlockSpec(x.shape, lambda n=len(x.shape): (0,) * n) for x in arrays]


def fetched(pairs, sems):
    copies = [pltpu.make_async_copy(a, b, sems.at[i]) for i, (a, b) in enumerate(pairs)]
    for copy in copies:
        copy.start()
    return copies


def pack_kernel(
    k_ref, v_ref, o_ref, lse_ref, delta_ref, docs_ref, gain_ref, kv_out, o_out, gain_out,
    lse_sc, delta_sc, docs_sc, sems,
):
    tokens, width = k_ref.shape
    copies = fetched(
        [
            (docs_ref, docs_sc),
            (lse_ref, lse_sc),
            (delta_ref, delta_sc),
            (k_ref, kv_out.at[:tokens]),
            (v_ref, kv_out.at[tokens : 2 * tokens]),
            (o_ref, o_out.at[:tokens]),
            (gain_ref, gain_out),
        ],
        sems,
    )
    for copy in copies[:3]:
        copy.wait()
    docs = (docs_sc[...] + 1).astype(F32)
    spare = kv_out.shape[0] - 2 * tokens - docs.shape[0]
    kv_out[2 * tokens :] = jnp.concatenate(
        [docs] + [jnp.zeros((spare, width), F32)] * (spare > 0)
    ).astype(BF)
    rows = []
    for ref in (lse_sc, delta_sc):
        rest = ref[...]
        for _ in range(3):
            piece = rest.astype(BF).astype(F32)
            rows.append(piece)
            rest = rest - piece
    rows.append(docs)
    spare = o_out.shape[0] - tokens - 7 * docs.shape[0]
    o_out[tokens:] = jnp.concatenate(
        rows + [jnp.zeros((spare, width), F32)] * (spare > 0)
    ).astype(BF)
    for copy in copies[3:]:
        copy.wait()


def query_kernel(parts, f_ref, h_ref, gain_ref, *refs):
    w_refs, (query_out, q_pre_out, w_out) = refs[:parts], refs[parts:]
    rows = w_refs[0].shape[0]
    q_pre = jnp.zeros(q_pre_out.shape, F32)
    for k in range(parts):
        at = pl.multiple_of((f_ref[0] - k + parts) % parts * rows, rows)
        q_pre += dot_nn(h_ref[:, pl.ds(at, rows)], w_refs[k][...])
        w_out[pl.ds(at, rows), :] = w_refs[k][...]
    inverse = lax.rsqrt(jnp.mean(q_pre * q_pre, axis=-1, keepdims=True) + 1e-06)
    q_pre_out[...] = q_pre
    query_out[...] = (q_pre * inverse * gain_ref[...]).astype(BF)


def row_data(o_ref, tokens, per):
    aux = o_ref[tokens:].astype(F32)
    part = []
    for at in range(0, 7 * per, per):
        part.append(
            jnp.concatenate([aux[at + j : at + j + 1, :] for j in range(per)], axis=1)
        )
    lse = (part[0] + part[1] + part[2]) * LOG2E
    return lse, part[3] + part[4] + part[5], part[6]


def stage_keys(kv_ref, s, tokens, width, k_sc, v_sc, kt_sc, docs_sc, with_kt):
    k_sc[s] = kv_ref[:tokens]
    v_sc[s] = kv_ref[tokens : 2 * tokens]
    if with_kt:
        kt_sc[s] = kv_ref[:tokens].astype(F32).T.astype(BF)
    docs = kv_ref[2 * tokens :].astype(F32)
    for j in range(tokens // width):
        row = jnp.broadcast_to(docs[j : j + 1, :], (width, width))
        docs_sc[s, j * width : (j + 1) * width, :] = row.T


def probabilities(s, rows, c, q, o, lse, delta, docs_q, diagonal, scale, k_sc, v_sc, docs_sc):
    scores = dot_nt(k_sc[s, rows, :], q)
    grad_prob = dot_nt(v_sc[s, rows, :], o)
    allowed = docs_sc[s, rows, :1] == docs_q
    if diagonal:
        t_at = c + lax.broadcasted_iota(jnp.int32, scores.shape, 0)
        i_at = lax.broadcasted_iota(jnp.int32, scores.shape, 1)
        allowed = allowed & (t_at <= i_at)
    prob = jnp.where(allowed, jnp.exp2(scores * (scale * LOG2E) - lse), 0.0)
    return prob, (prob * (grad_prob - delta)).astype(BF)


def slot(r, k, j, far):
    if j > 0:
        return j
    return 0 if k == 0 else jnp.where(r >= k, far, 0)


def others_kernel(group, far, tokens, width, r_ref, q_ref, *refs):
    o_refs, kv_refs = refs[: group - 1], refs[group - 1 : group + far]
    outs = refs[group + far :]
    dq_refs, dkv_ref, acc = outs[: group - 1], outs[group - 1], outs[group]
    kt_sc, docs_sc, k_sc, v_sc = outs[group + 1 :]
    r = r_ref[0]
    scale = width ** (-0.5)
    for s in range(far + 1):
        stage_keys(kv_refs[s], s, tokens, width, k_sc, v_sc, kt_sc, docs_sc, True)
        acc[s] = jnp.zeros((2 * tokens, width), F32)
    for k in range(1, group):
        q = q_ref[(r - k + group) % group]
        o = o_refs[k - 1][:tokens]
        lse, delta, docs_q = row_data(o_refs[k - 1], tokens, tokens // width)
        dqt = jnp.zeros((width, tokens), F32)
        for j in range(far):
            s = slot(r, k, j, far)
            for c in range(0, tokens, T_CHUNK):
                rows = slice(c, c + T_CHUNK)
                below = slice(tokens + c, tokens + c + T_CHUNK)
                prob, dscore = probabilities(
                    s, rows, c, q, o, lse, delta, docs_q, False, scale, k_sc, v_sc, docs_sc
                )
                acc[s, below, :] += dot_nn(prob.astype(BF), o)
                acc[s, rows, :] += dot_nn(dscore, q)
                dqt += dot_nn(kt_sc[s, :, rows], dscore)
        dq_refs[k - 1][...] = (dqt.T * scale).astype(BF)
    dkv_ref[:tokens] = (acc[far, :tokens] * scale).astype(BF)
    dkv_ref[tokens:] = acc[far, tokens:].astype(BF)


def own_kernel(far, tokens, width, q_ref, o_ref, acc, *refs):
    kv_refs, dq_ref, dkv_refs = refs[:far], refs[far], refs[far + 1 : 2 * far + 1]
    kt_sc, docs_sc, k_sc, v_sc = refs[2 * far + 1 :]
    scale = width ** (-0.5)
    q = q_ref[...]
    o = o_ref[:tokens]
    lse, delta, docs_q = row_data(o_ref, tokens, tokens // width)
    dqt = jnp.zeros((width, tokens), F32)
    for s in range(far):
        stage_keys(kv_refs[s], s, tokens, width, k_sc, v_sc, kt_sc, docs_sc, True)
        for c in range(0, tokens, T_CHUNK):
            rows = slice(c, c + T_CHUNK)
            below = slice(tokens + c, tokens + c + T_CHUNK)
            prob, dscore = probabilities(
                s, rows, c, q, o, lse, delta, docs_q, s == 0, scale, k_sc, v_sc, docs_sc
            )
            dkv_refs[s][below, :] = (acc[s, below, :] + dot_nn(prob.astype(BF), o)).astype(BF)
            dkv_refs[s][rows, :] = ((acc[s, rows, :] + dot_nn(dscore, q)) * scale).astype(BF)
            dqt += dot_nn(kt_sc[s, :, rows], dscore)
    dq_ref[...] = dqt.T * scale


def key_scratch(slots, tokens, width):
    return [
        pltpu.VMEM((slots, width, tokens), BF),
        pltpu.VMEM((slots, tokens, width), F32),
        pltpu.VMEM((slots, tokens, width), BF),
        pltpu.VMEM((slots, tokens, width), BF),
    ]


def cost(pairs, tokens, width):
    return pl.CostEstimate(
        flops=pairs * 10 * tokens * tokens * width,
        bytes_accessed=pairs * 8 * tokens * width,
        transcendentals=pairs * tokens * tokens,
    )


def others(group, far, tokens, width, r, q_all, o_list, kv_list):
    block = jax.ShapeDtypeStruct((tokens, width), BF)
    double = jax.ShapeDtypeStruct((2 * tokens, width), BF)
    sums = jax.ShapeDtypeStruct((far + 1, 2 * tokens, width), F32)
    if group == 1:
        return [], jnp.zeros(double.shape, BF), jnp.zeros(sums.shape, F32)
    out = pl.pallas_call(
        functools.partial(others_kernel, group, far, tokens, width),
        out_shape=[block] * (group - 1) + [double, sums],
        in_specs=[pl.BlockSpec(memory_space=pltpu.SMEM)] + vmem_specs(group + far + 1),
        out_specs=vmem_specs(group + 1),
        scratch_shapes=key_scratch(far + 1, tokens, width),
        compiler_params=params(ATTENTION_MIB),
        cost_estimate=cost((group - 1) * far, tokens, width),
        name="others",
    )(r, q_all, *o_list[1:], *kv_list)
    return out[: group - 1], out[group - 1], out[group]


def own(far, tokens, width, query, o_own, acc, kv_list):
    out = pl.pallas_call(
        functools.partial(own_kernel, far, tokens, width),
        out_shape=[jax.ShapeDtypeStruct((tokens, width), F32)]
        + [jax.ShapeDtypeStruct((2 * tokens, width), BF)] * far,
        in_specs=vmem_specs(far + 3),
        out_specs=vmem_specs(far + 1),
        scratch_shapes=key_scratch(far, tokens, width),
        compiler_params=params(ATTENTION_MIB),
        cost_estimate=cost(far, tokens, width),
        name="own",
    )(query, o_own, acc, *kv_list[:far])
    return out[0], out[1:]


def pre_kernel(parts, halves, f_ref, h_ref, q_pre_ref, gain_ref, own_ref, *refs):
    grad_query = own_ref[...]
    for ref in refs[:parts]:
        grad_query = grad_query + ref[...].astype(F32)
    pre_out, turned_out, give_refs = refs[parts], refs[parts + 1], refs[parts + 2 :]
    q_pre = q_pre_ref[...]
    inverse = lax.rsqrt(jnp.mean(q_pre * q_pre, axis=-1, keepdims=True) + 1e-06)
    normed = q_pre * inverse
    scaled = grad_query * gain_ref[...]
    grad_pre = inverse * (scaled - normed * jnp.mean(scaled * normed, axis=-1, keepdims=True))
    grad_pre = grad_pre.astype(BF)
    pre_out[...] = grad_pre
    turned_pre = grad_pre.astype(F32).T.astype(BF)
    turned_out[...] = turned_pre
    for k in range(1, halves):
        rows_of_term(turned_pre, h_ref, (f_ref[0] + k) % halves, give_refs[k - 1])


def keep_kernel(f_ref, h_ref, turned_ref, keep_ref):
    rows_of_term(turned_ref[...], h_ref, f_ref[0], keep_ref)


def rows_of_term(turned_pre, h_ref, owner, out_ref):
    rows = out_ref.shape[0]
    chunk = math.gcd(rows, 512)
    for c in range(0, rows, chunk):
        at = pl.multiple_of(owner * rows + c, chunk)
        term = dot_nn(turned_pre, h_ref[:, pl.ds(at, chunk)])
        out_ref[c : c + chunk, :] = term.T.astype(out_ref.dtype)


def add_kernel(keep_ref, *refs):
    total = keep_ref[...]
    for ref in refs[:-1]:
        total = total + ref[...].astype(F32)
    refs[-1][...] = total.astype(BF)


def sum_kernel(got_ref, out_ref):
    total = got_ref[0].astype(F32)
    for i in range(1, got_ref.shape[0]):
        total = total + got_ref[i].astype(F32)
    total = total.astype(BF)
    for i in range(out_ref.shape[0]):
        out_ref[i] = total


def sum_and_repeat(got, copies):
    share, width = got.shape[1:]
    if share % 16:
        total = jnp.sum(got.astype(F32), axis=0).astype(BF)
        return jnp.broadcast_to(total[None], (copies, share, width))
    return pl.pallas_call(
        sum_kernel,
        out_shape=jax.ShapeDtypeStruct((copies, share, width), BF),
        in_specs=vmem_specs(1),
        out_specs=vmem_specs(1)[0],
        compiler_params=params(8),
        name="sum_and_repeat",
    )(got)


def local(
    hidden_in, w_query, query_gain, key_rows, value_rows, grad_out, logsumexp, row_delta, doc_ids
):
    return step(
        hidden_in[0],
        w_query,
        query_gain[None],
        key_rows[0],
        value_rows[0],
        grad_out[0],
        logsumexp,
        row_delta,
        doc_ids,
    )


def step(inputs, w_query, gain, keys, values, outgrad, logsumexp, row_delta, doc_ids):
    tokens, width = keys.shape
    blocks = lax.axis_size("blk")
    halves = lax.axis_size("fsdp")
    group = math.gcd(blocks, max(1, ROUNDS // 2))
    far = ROUNDS // group
    r = (lax.axis_index("blk") % group).astype(jnp.int32)[None]
    per = tokens // width

    w_parts = [w_query] + [
        lax.ppermute(w_query, "fsdp", [(i, (i + k) % halves) for i in range(halves)])
        for k in range(1, halves)
    ]
    kv_own, o_own, gain = pl.pallas_call(
        pack_kernel,
        out_shape=[
            jax.ShapeDtypeStruct((2 * tokens + -(-per // 16) * 16, width), BF),
            jax.ShapeDtypeStruct((tokens + -(-7 * per // 16) * 16, width), BF),
            jax.ShapeDtypeStruct(gain.shape, F32),
        ],
        in_specs=hbm_specs(7),
        out_specs=vmem_specs(3),
        scratch_shapes=[
            pltpu.VMEM((per, width), F32),
            pltpu.VMEM((per, width), F32),
            pltpu.VMEM((per, width), jnp.int32),
            pltpu.SemaphoreType.DMA((7,)),
        ],
        compiler_params=params(PACK_MIB),
        name="pack",
    )(
        keys,
        values,
        outgrad,
        logsumexp.reshape(per, width),
        row_delta.reshape(per, width),
        doc_ids.reshape(per, width),
        gain,
    )
    kv_list = [kv_own]
    for _ in range(1, far + 1):
        kv_list.append(shifted(kv_list[-1], group))
    o_list = [o_own] + [turned(o_own, k, group) for k in range(1, group)]

    f = lax.axis_index("fsdp").astype(jnp.int32)[None]
    q_like = jax.ShapeDtypeStruct((tokens, width), F32)
    w_like = jax.ShapeDtypeStruct((inputs.shape[1], width), BF)
    query, q_pre, projection = pl.pallas_call(
        functools.partial(query_kernel, halves),
        out_shape=[jax.ShapeDtypeStruct((tokens, width), BF), q_like, w_like],
        in_specs=[pl.BlockSpec(memory_space=pltpu.SMEM)]
        + vmem_specs(2)
        + whole_specs(w_parts),
        out_specs=vmem_specs(1) + whole_specs([q_like, w_like]),
        compiler_params=params(8),
        name="query",
    )(f, inputs, gain, *w_parts)
    groups = [list(range(i, i + group)) for i in range(0, blocks, group)]
    q_all = lax.all_gather(query, "blk", axis_index_groups=groups)

    dq_list, grad_kv, acc = others(group, far, tokens, width, r, q_all, o_list, kv_list)

    dq_back = [turned(dq_list[k - 1], -k, group) for k in range(1, group)]
    back = shifted(grad_kv, -group)
    dq_own, dkv_list = own(far, tokens, width, query, o_own, acc, kv_list)
    owned = inputs.shape[1] // halves
    smem = [pl.BlockSpec(memory_space=pltpu.SMEM)]
    block = jax.ShapeDtypeStruct((tokens, width), BF)
    turned_block = jax.ShapeDtypeStruct((width, tokens), BF)
    rows = jax.ShapeDtypeStruct((owned, width), BF)
    grad_pre, turned_pre, *give = pl.pallas_call(
        functools.partial(pre_kernel, len(dq_back), halves),
        out_shape=[block, turned_block] + [rows] * (halves - 1),
        in_specs=smem
        + vmem_specs(1)
        + whole_specs([q_pre, gain])
        + vmem_specs(1 + len(dq_back)),
        out_specs=vmem_specs(1 + halves),
        compiler_params=params(16),
        name="give_term",
    )(f, inputs, q_pre, gain, dq_own, *dq_back)
    got = [
        lax.ppermute(give[k - 1], "fsdp", [(i, (i + k) % halves) for i in range(halves)])
        for k in range(1, halves)
    ]
    keep = pl.pallas_call(
        keep_kernel,
        out_shape=jax.ShapeDtypeStruct((owned, width), F32),
        in_specs=smem + vmem_specs(2),
        out_specs=vmem_specs(1)[0],
        compiler_params=params(16),
        cost_estimate=pl.CostEstimate(
            flops=2 * tokens * owned * width, bytes_accessed=2 * tokens * owned, transcendentals=0
        ),
        name="keep_term",
    )(f, inputs, turned_pre)
    terms = pl.pallas_call(
        add_kernel,
        out_shape=rows,
        in_specs=vmem_specs(halves),
        out_specs=vmem_specs(1)[0],
        compiler_params=params(8),
        name="add_terms",
    )(keep, *got)
    grad_hidden = dot_nt(grad_pre, projection).astype(BF)

    for s in range(far - 1, -1, -1):
        grad_kv = (dkv_list[s].astype(F32) + back.astype(F32)).astype(BF)
        if s > 0:
            back = shifted(grad_kv, -group)

    share = -(-owned // blocks)
    if share * blocks != owned:
        terms = jnp.pad(terms, ((0, share * blocks - owned), (0, 0)))
    got = lax.all_to_all(terms, "blk", 0, 0, tiled=True)
    everywhere = sum_and_repeat(got.reshape(blocks, share, width), blocks)
    total = lax.all_to_all(everywhere.reshape(-1, width), "blk", 0, 0, tiled=True)
    grad_wquery = total[:owned].astype(F32)
    return (grad_hidden[None], grad_kv[None, :tokens], grad_kv[None, tokens:], grad_wquery)


def solution(mesh):
    return jax.shard_map(
        local,
        mesh=mesh,
        in_specs=(
            P("fsdp", "blk", None),
            P("fsdp", None),
            P(),
            P("fsdp", "blk", None),
            P("fsdp", "blk", None),
            P("fsdp", "blk", None),
            P("fsdp", "blk"),
            P("fsdp", "blk"),
            P("fsdp", "blk"),
        ),
        out_specs=(
            P("fsdp", "blk", None),
            P("fsdp", "blk", None),
            P("fsdp", "blk", None),
            P("fsdp", None),
        ),
        check_vma=False,
    )
```

```python
import functools
import math

import jax
import jax.numpy as jnp
from jax import lax
from jax.experimental import pallas as pl
from jax.experimental.pallas import tpu as pltpu
from jax.sharding import PartitionSpec as P


ROUNDS = 8
LOG2E = 1.4426950408889634
BF = jnp.bfloat16
F32 = jnp.float32
T_CHUNK = 256
PACK_MIB = 63.4
ATTENTION_MIB = 16


def shifted(value, by):
    size = lax.axis_size("blk")
    pairs = [(i, i + by) for i in range(size) if 0 <= i + by < size]
    return lax.ppermute(value, "blk", pairs)


def turned(value, by, group):
    size = lax.axis_size("blk")
    pairs = [(i, i - i % group + (i + by) % group) for i in range(size)]
    return lax.ppermute(value, "blk", pairs)


def vmem_specs(count):
    return [pl.BlockSpec(memory_space=pltpu.VMEM)] * count


def params(mib):
    return pltpu.CompilerParams(vmem_limit_bytes=int(mib * 1024 * 1024))


def dot_nt(a, b):
    return lax.dot_general(a, b, (((1,), (1,)), ((), ())), preferred_element_type=F32)


def dot_nn(a, b):
    return lax.dot_general(a, b, (((1,), (0,)), ((), ())), preferred_element_type=F32)


def hbm_specs(count):
    return [pl.BlockSpec(memory_space=pltpu.HBM)] * count


def whole_specs(arrays):
    return [pl.BlockSpec(x.shape, lambda n=len(x.shape): (0,) * n) for x in arrays]


def fetched(pairs, sems):
    copies = [pltpu.make_async_copy(a, b, sems.at[i]) for i, (a, b) in enumerate(pairs)]
    for copy in copies:
        copy.start()
    return copies


def pack_kernel(
    k_ref, v_ref, o_ref, lse_ref, delta_ref, docs_ref, gain_ref, kv_out, o_out, gain_out,
    lse_sc, delta_sc, docs_sc, sems,
):
    tokens, width = k_ref.shape
    copies = fetched(
        [
            (docs_ref, docs_sc),
            (lse_ref, lse_sc),
            (delta_ref, delta_sc),
            (k_ref, kv_out.at[:tokens]),
            (v_ref, kv_out.at[tokens : 2 * tokens]),
            (o_ref, o_out.at[:tokens]),
            (gain_ref, gain_out),
        ],
        sems,
    )
    for copy in copies[:3]:
        copy.wait()
    docs = (docs_sc[...] + 1).astype(F32)
    spare = kv_out.shape[0] - 2 * tokens - docs.shape[0]
    kv_out[2 * tokens :] = jnp.concatenate(
        [docs] + [jnp.zeros((spare, width), F32)] * (spare > 0)
    ).astype(BF)
    rows = []
    for ref in (lse_sc, delta_sc):
        rest = ref[...]
        for _ in range(3):
            piece = rest.astype(BF).astype(F32)
            rows.append(piece)
            rest = rest - piece
    rows.append(docs)
    spare = o_out.shape[0] - tokens - 7 * docs.shape[0]
    o_out[tokens:] = jnp.concatenate(
        rows + [jnp.zeros((spare, width), F32)] * (spare > 0)
    ).astype(BF)
    for copy in copies[3:]:
        copy.wait()


def query_kernel(parts, f_ref, h_ref, gain_ref, *refs):
    w_refs, (query_out, q_pre_out, w_out) = refs[:parts], refs[parts:]
    rows = w_refs[0].shape[0]
    q_pre = jnp.zeros(q_pre_out.shape, F32)
    for k in range(parts):
        at = pl.multiple_of((f_ref[0] - k + parts) % parts * rows, rows)
        q_pre += dot_nn(h_ref[:, pl.ds(at, rows)], w_refs[k][...])
        w_out[pl.ds(at, rows), :] = w_refs[k][...]
    inverse = lax.rsqrt(jnp.mean(q_pre * q_pre, axis=-1, keepdims=True) + 1e-06)
    q_pre_out[...] = q_pre
    query_out[...] = (q_pre * inverse * gain_ref[...]).astype(BF)


def row_data(o_ref, tokens, per):
    aux = o_ref[tokens:].astype(F32)
    part = []
    for at in range(0, 7 * per, per):
        part.append(
            jnp.concatenate([aux[at + j : at + j + 1, :] for j in range(per)], axis=1)
        )
    lse = (part[0] + part[1] + part[2]) * LOG2E
    return lse, part[3] + part[4] + part[5], part[6]


def stage_keys(kv_ref, s, tokens, width, k_sc, v_sc, kt_sc, docs_sc, with_kt):
    k_sc[s] = kv_ref[:tokens]
    v_sc[s] = kv_ref[tokens : 2 * tokens]
    if with_kt:
        kt_sc[s] = kv_ref[:tokens].astype(F32).T.astype(BF)
    docs = kv_ref[2 * tokens :].astype(F32)
    for j in range(tokens // width):
        row = jnp.broadcast_to(docs[j : j + 1, :], (width, width))
        docs_sc[s, j * width : (j + 1) * width, :] = row.T


def probabilities(s, rows, c, q, o, lse, delta, docs_q, diagonal, scale, k_sc, v_sc, docs_sc):
    scores = dot_nt(k_sc[s, rows, :], q)
    grad_prob = dot_nt(v_sc[s, rows, :], o)
    allowed = docs_sc[s, rows, :1] == docs_q
    if diagonal:
        t_at = c + lax.broadcasted_iota(jnp.int32, scores.shape, 0)
        i_at = lax.broadcasted_iota(jnp.int32, scores.shape, 1)
        allowed = allowed & (t_at <= i_at)
    prob = jnp.where(allowed, jnp.exp2(scores * (scale * LOG2E) - lse), 0.0)
    return prob, (prob * (grad_prob - delta)).astype(BF)


def slot(r, k, j, far):
    if j > 0:
        return j
    return 0 if k == 0 else jnp.where(r >= k, far, 0)


def others_kernel(group, far, tokens, width, r_ref, sums_ref, *refs):
    q_refs, o_refs = refs[: group - 1], refs[group - 1 : 2 * group - 2]
    kv_refs = refs[2 * group - 2 : 2 * group + far - 1]
    outs = refs[2 * group + far - 1 :]
    dq_refs, dkv_refs = outs[: group - 1], outs[group - 1 : group + far]
    kt_sc, docs_sc, k_sc, v_sc, acc = outs[group + far :]
    r = r_ref[0]
    scale = width ** (-0.5)
    for s in range(far + 1):
        stage_keys(kv_refs[s], s, tokens, width, k_sc, v_sc, kt_sc, docs_sc, True)
        acc[s] = sums_ref[s] if s < far else jnp.zeros((2 * tokens, width), F32)
    for k in range(1, group):
        q = q_refs[k - 1][...]
        o = o_refs[k - 1][:tokens]
        lse, delta, docs_q = row_data(o_refs[k - 1], tokens, tokens // width)
        dqt = jnp.zeros((width, tokens), F32)
        for j in range(far):
            s = slot(r, k, j, far)
            for c in range(0, tokens, T_CHUNK):
                rows = slice(c, c + T_CHUNK)
                below = slice(tokens + c, tokens + c + T_CHUNK)
                prob, dscore = probabilities(
                    s, rows, c, q, o, lse, delta, docs_q, False, scale, k_sc, v_sc, docs_sc
                )
                acc[s, below, :] += dot_nn(prob.astype(BF), o)
                acc[s, rows, :] += dot_nn(dscore, q)
                dqt += dot_nn(kt_sc[s, :, rows], dscore)
        dq_refs[k - 1][...] = (dqt.T * scale).astype(BF)
    for s in range(far + 1):
        dkv_refs[s][:tokens] = (acc[s, :tokens] * scale).astype(BF)
        dkv_refs[s][tokens:] = acc[s, tokens:].astype(BF)


def own_kernel(far, tokens, width, q_ref, o_ref, *refs):
    kv_refs, dq_ref, sums_ref = refs[:far], refs[far], refs[far + 1]
    kt_sc, docs_sc, k_sc, v_sc = refs[far + 2 :]
    scale = width ** (-0.5)
    q = q_ref[...]
    o = o_ref[:tokens]
    lse, delta, docs_q = row_data(o_ref, tokens, tokens // width)
    dqt = jnp.zeros((width, tokens), F32)
    for s in range(far):
        stage_keys(kv_refs[s], s, tokens, width, k_sc, v_sc, kt_sc, docs_sc, True)
        for c in range(0, tokens, T_CHUNK):
            rows = slice(c, c + T_CHUNK)
            below = slice(tokens + c, tokens + c + T_CHUNK)
            prob, dscore = probabilities(
                s, rows, c, q, o, lse, delta, docs_q, s == 0, scale, k_sc, v_sc, docs_sc
            )
            sums_ref[s, below, :] = dot_nn(prob.astype(BF), o)
            sums_ref[s, rows, :] = dot_nn(dscore, q)
            dqt += dot_nn(kt_sc[s, :, rows], dscore)
    dq_ref[...] = dqt.T * scale


def key_scratch(slots, tokens, width):
    return [
        pltpu.VMEM((slots, width, tokens), BF),
        pltpu.VMEM((slots, tokens, width), F32),
        pltpu.VMEM((slots, tokens, width), BF),
        pltpu.VMEM((slots, tokens, width), BF),
    ]


def cost(pairs, tokens, width):
    return pl.CostEstimate(
        flops=pairs * 10 * tokens * tokens * width,
        bytes_accessed=pairs * 8 * tokens * width,
        transcendentals=pairs * tokens * tokens,
    )


def others(group, far, tokens, width, r, sums, q_list, o_list, kv_list):
    block = jax.ShapeDtypeStruct((tokens, width), BF)
    double = jax.ShapeDtypeStruct((2 * tokens, width), BF)
    out = pl.pallas_call(
        functools.partial(others_kernel, group, far, tokens, width),
        out_shape=[block] * (group - 1) + [double] * (far + 1),
        in_specs=[pl.BlockSpec(memory_space=pltpu.SMEM)] + vmem_specs(2 * group + far),
        out_specs=vmem_specs(group + far),
        scratch_shapes=key_scratch(far + 1, tokens, width)
        + [pltpu.VMEM((far + 1, 2 * tokens, width), F32)],
        compiler_params=params(ATTENTION_MIB),
        cost_estimate=cost(max(1, (group - 1) * far), tokens, width),
        name="others",
    )(r, sums, *q_list[1:], *o_list[1:], *kv_list)
    return out[: group - 1], out[group - 1 :]


def own(far, tokens, width, query, o_own, kv_list):
    return pl.pallas_call(
        functools.partial(own_kernel, far, tokens, width),
        out_shape=[
            jax.ShapeDtypeStruct((tokens, width), F32),
            jax.ShapeDtypeStruct((far, 2 * tokens, width), F32),
        ],
        in_specs=vmem_specs(far + 2),
        out_specs=vmem_specs(2),
        scratch_shapes=key_scratch(far, tokens, width),
        compiler_params=params(ATTENTION_MIB),
        cost_estimate=cost(far, tokens, width),
        name="own",
    )(query, o_own, *kv_list[:far])


def pre_kernel(parts, halves, f_ref, h_ref, q_pre_ref, gain_ref, own_ref, *refs):
    grad_query = own_ref[...]
    for ref in refs[:parts]:
        grad_query = grad_query + ref[...].astype(F32)
    pre_out, turned_out, give_refs = refs[parts], refs[parts + 1], refs[parts + 2 :]
    q_pre = q_pre_ref[...]
    inverse = lax.rsqrt(jnp.mean(q_pre * q_pre, axis=-1, keepdims=True) + 1e-06)
    normed = q_pre * inverse
    scaled = grad_query * gain_ref[...]
    grad_pre = inverse * (scaled - normed * jnp.mean(scaled * normed, axis=-1, keepdims=True))
    grad_pre = grad_pre.astype(BF)
    pre_out[...] = grad_pre
    turned_pre = grad_pre.astype(F32).T.astype(BF)
    turned_out[...] = turned_pre
    for k in range(1, halves):
        rows_of_term(turned_pre, h_ref, (f_ref[0] + k) % halves, give_refs[k - 1])


def keep_kernel(f_ref, h_ref, turned_ref, keep_ref):
    rows_of_term(turned_ref[...], h_ref, f_ref[0], keep_ref)


def rows_of_term(turned_pre, h_ref, owner, out_ref):
    rows = out_ref.shape[0]
    chunk = math.gcd(rows, 512)
    for c in range(0, rows, chunk):
        at = pl.multiple_of(owner * rows + c, chunk)
        term = dot_nn(turned_pre, h_ref[:, pl.ds(at, chunk)])
        out_ref[c : c + chunk, :] = term.T.astype(out_ref.dtype)


def add_kernel(keep_ref, *refs):
    total = keep_ref[...]
    for ref in refs[:-1]:
        total = total + ref[...].astype(F32)
    refs[-1][...] = total.astype(BF)


def sum_kernel(got_ref, out_ref):
    total = got_ref[0].astype(F32)
    for i in range(1, got_ref.shape[0]):
        total = total + got_ref[i].astype(F32)
    total = total.astype(BF)
    for i in range(out_ref.shape[0]):
        out_ref[i] = total


def sum_and_repeat(got, copies):
    share, width = got.shape[1:]
    if share % 16:
        total = jnp.sum(got.astype(F32), axis=0).astype(BF)
        return jnp.broadcast_to(total[None], (copies, share, width))
    return pl.pallas_call(
        sum_kernel,
        out_shape=jax.ShapeDtypeStruct((copies, share, width), BF),
        in_specs=vmem_specs(1),
        out_specs=vmem_specs(1)[0],
        compiler_params=params(8),
        name="sum_and_repeat",
    )(got)


def local(
    hidden_in, w_query, query_gain, key_rows, value_rows, grad_out, logsumexp, row_delta, doc_ids
):
    return step(
        hidden_in[0],
        w_query,
        query_gain[None],
        key_rows[0],
        value_rows[0],
        grad_out[0],
        logsumexp,
        row_delta,
        doc_ids,
    )


def step(inputs, w_query, gain, keys, values, outgrad, logsumexp, row_delta, doc_ids):
    tokens, width = keys.shape
    blocks = lax.axis_size("blk")
    halves = lax.axis_size("fsdp")
    group = math.gcd(blocks, max(1, ROUNDS // 2))
    far = ROUNDS // group
    r = (lax.axis_index("blk") % group).astype(jnp.int32)[None]
    per = tokens // width

    w_parts = [w_query] + [
        lax.ppermute(w_query, "fsdp", [(i, (i + k) % halves) for i in range(halves)])
        for k in range(1, halves)
    ]
    kv_own, o_own, gain = pl.pallas_call(
        pack_kernel,
        out_shape=[
            jax.ShapeDtypeStruct((2 * tokens + -(-per // 16) * 16, width), BF),
            jax.ShapeDtypeStruct((tokens + -(-7 * per // 16) * 16, width), BF),
            jax.ShapeDtypeStruct(gain.shape, F32),
        ],
        in_specs=hbm_specs(7),
        out_specs=vmem_specs(3),
        scratch_shapes=[
            pltpu.VMEM((per, width), F32),
            pltpu.VMEM((per, width), F32),
            pltpu.VMEM((per, width), jnp.int32),
            pltpu.SemaphoreType.DMA((7,)),
        ],
        compiler_params=params(PACK_MIB),
        name="pack",
    )(
        keys,
        values,
        outgrad,
        logsumexp.reshape(per, width),
        row_delta.reshape(per, width),
        doc_ids.reshape(per, width),
        gain,
    )
    kv_list = [kv_own]
    for _ in range(1, far + 1):
        kv_list.append(shifted(kv_list[-1], group))
    o_list = [o_own] + [turned(o_own, k, group) for k in range(1, group)]

    f = lax.axis_index("fsdp").astype(jnp.int32)[None]
    q_like = jax.ShapeDtypeStruct((tokens, width), F32)
    w_like = jax.ShapeDtypeStruct((inputs.shape[1], width), BF)
    query, q_pre, projection = pl.pallas_call(
        functools.partial(query_kernel, halves),
        out_shape=[jax.ShapeDtypeStruct((tokens, width), BF), q_like, w_like],
        in_specs=[pl.BlockSpec(memory_space=pltpu.SMEM)]
        + vmem_specs(2)
        + whole_specs(w_parts),
        out_specs=vmem_specs(1) + whole_specs([q_like, w_like]),
        compiler_params=params(8),
        name="query",
    )(f, inputs, gain, *w_parts)
    q_list = [query] + [turned(query, k, group) for k in range(1, group)]
    dq_own, sums = own(far, tokens, width, query, o_own, kv_list)
    dq_list, dkv_list = others(
        group, far, tokens, width, r, sums, q_list, o_list, kv_list
    )

    dq_back = [turned(dq_list[k - 1], -k, group) for k in range(1, group)]
    back = shifted(dkv_list[far], -group)
    owned = inputs.shape[1] // halves
    smem = [pl.BlockSpec(memory_space=pltpu.SMEM)]
    block = jax.ShapeDtypeStruct((tokens, width), BF)
    turned_block = jax.ShapeDtypeStruct((width, tokens), BF)
    rows = jax.ShapeDtypeStruct((owned, width), BF)
    grad_pre, turned_pre, *give = pl.pallas_call(
        functools.partial(pre_kernel, len(dq_back), halves),
        out_shape=[block, turned_block] + [rows] * (halves - 1),
        in_specs=smem
        + vmem_specs(1)
        + whole_specs([q_pre, gain])
        + vmem_specs(1 + len(dq_back)),
        out_specs=vmem_specs(1 + halves),
        compiler_params=params(16),
        name="give_term",
    )(f, inputs, q_pre, gain, dq_own, *dq_back)
    got = [
        lax.ppermute(give[k - 1], "fsdp", [(i, (i + k) % halves) for i in range(halves)])
        for k in range(1, halves)
    ]
    keep = pl.pallas_call(
        keep_kernel,
        out_shape=jax.ShapeDtypeStruct((owned, width), F32),
        in_specs=smem + vmem_specs(2),
        out_specs=vmem_specs(1)[0],
        compiler_params=params(16),
        cost_estimate=pl.CostEstimate(
            flops=2 * tokens * owned * width, bytes_accessed=2 * tokens * owned, transcendentals=0
        ),
        name="keep_term",
    )(f, inputs, turned_pre)
    terms = pl.pallas_call(
        add_kernel,
        out_shape=rows,
        in_specs=vmem_specs(halves),
        out_specs=vmem_specs(1)[0],
        compiler_params=params(8),
        name="add_terms",
    )(keep, *got)
    grad_hidden = dot_nt(grad_pre, projection).astype(BF)

    for s in range(far - 1, -1, -1):
        grad_kv = (dkv_list[s].astype(F32) + back.astype(F32)).astype(BF)
        if s > 0:
            back = shifted(grad_kv, -group)

    share = -(-owned // blocks)
    if share * blocks != owned:
        terms = jnp.pad(terms, ((0, share * blocks - owned), (0, 0)))
    got = lax.all_to_all(terms, "blk", 0, 0, tiled=True)
    everywhere = sum_and_repeat(got.reshape(blocks, share, width), blocks)
    total = lax.all_to_all(everywhere.reshape(-1, width), "blk", 0, 0, tiled=True)
    grad_wquery = total[:owned].astype(F32)
    return (grad_hidden[None], grad_kv[None, :tokens], grad_kv[None, tokens:], grad_wquery)


def solution(mesh):
    return jax.shard_map(
        local,
        mesh=mesh,
        in_specs=(
            P("fsdp", "blk", None),
            P("fsdp", None),
            P(),
            P("fsdp", "blk", None),
            P("fsdp", "blk", None),
            P("fsdp", "blk", None),
            P("fsdp", "blk"),
            P("fsdp", "blk"),
            P("fsdp", "blk"),
        ),
        out_specs=(
            P("fsdp", "blk", None),
            P("fsdp", "blk", None),
            P("fsdp", "blk", None),
            P("fsdp", None),
        ),
        check_vma=False,
    )
```
